128 devices in a mesh: lat: 16 (over z, x), lon: 8 (over y, core).
Axes of the slice: x: 4, y: 4, z: 4, core: 2. Of those that a mesh axis runs over, the one named last changes fastest.
Arguments:
- grid_feat: bfloat16 [131072, 474], P(('lat', 'lon')), may hold values from -6 to 6
- grid_send: int32 [128, 4, 256], P(('lat', 'lon')), may hold values from 0 to 1023
- g2m_sender: int32 [524288], P(('lat', 'lon')), may hold values from 0 to 2047, as said below
- g2m_receiver: int32 [524288], P(('lat', 'lon')), may hold values from 0 to 320, as said below
- g2m_geom: float32 [4, 524288], P(None, ('lat', 'lon')), may hold values from -1 to 1
- mesh_geom: float32 [3, 40960], P(None, ('lat', 'lon')), may hold values from -1 to 1
- mesh_adjacent_lists: int32 [128, 8, 112], P(('lat', 'lon')), may hold values from 0 to 319
- mesh_far: int32 [128, 128, 4], P(('lat', 'lon')), may hold values from 0 to 319
- mesh_sender: int32 [524288], P(('lat', 'lon')), may hold values from 0 to 1727, as said below
- mesh_receiver: int32 [524288], P(('lat', 'lon')), may hold values from 0 to 320, as said below
- mesh_edge_geom: float32 [4, 524288], P(None, ('lat', 'lon')), may hold values from -1 to 1
- embed_in: bfloat16 [474, 512], replicated, may hold values from -0.25 to 0.25
- mesh_in: float32 [3, 512], replicated, may hold values from -3.5 to 3.5
- geo_in: float32 [3, 4, 512], replicated, may hold values from -3 to 3
- pair_in: bfloat16 [3, 4, 512, 512], replicated, may hold values from -0.1875 to 0.1875
- square_out: bfloat16 [8, 512, 512], replicated, may hold values from -0.25 to 0.25
Outputs:
- mesh_out: bfloat16 [40960, 512], P(('lat', 'lon'))
The draws below stay inside these ranges and needn't reach their ends.
Inputs may be any that keep to these rules, and one draw needn't show every extreme that they name: grid_send[s, d, k] is a local grid row of device s, which it sends to the device that has s as its source for side offset o_d. `g2m_sender`: below 1024, a local grid row of the edge's device; else 1024 + d * 256 + k, a row of received_grid whose source exists. `g2m_receiver`: a local mesh row of the edge's device, or 320 for a padding edge; a device's live edges come first, and some device has all 4096 live. mesh_adjacent_lists[t, d, k] is a local mesh row of device t, which it sends to the device that has t as its source for neighbour offset n_d. mesh_far[t, q, k] is a local mesh row of device t, which it sends to device q. `mesh_sender`: below 320, a local mesh row of the edge's device; else a halo row of the edge's device, and a neighbour's row only where that neighbour exists. `mesh_receiver`: a local mesh row of the edge's device, or 320 for a padding edge; a device's live edges come first, and some device has all 4096 live.
All inputs are finite; a program needn't handle non-finite values.
Results may differ from the reference program's by a relative error of at most 0.015.
Values may be sent and summed in bfloat16 or wider, within the bound.
A program may use at most 128 MiB of HBM per device.

```python
import jax
import jax.numpy as jnp
from jax import lax

D = 512
C_IN = 474
GRID_DEV = 1024
GSLOT = 256
MESH_PER_DEVICE = 320
NEAR_ROW_SLOTS = 112
FAR_ROW_SLOTS = 4
E_G2M = 4096
E_MESH = 4096
STEPS = 2
GRID = 131072
MESH = 40960
G2M = 524288
MESH_EDGE_SLOTS = 524288
SECTIONS = 3
SQUARES = 8
N_LAT = 16
N_LON = 8
DEVICES = 128


GRID_LAT_STEPS = (-1, 1, 0, 0)


MESH_LATITUDES = (-1, -1, -1, 0, 0, 1, 1, 1)


def live_mask(seed_key, device_row_total, per_device):
    shifts = jax.random.randint(jax.random.fold_in(seed_key, 11), (device_row_total,), 0, 3)
    tallies = jnp.right_shift(jnp.full((device_row_total,), per_device, jnp.int32), shifts.astype(jnp.int32))
    fullest_device = jax.random.randint(jax.random.fold_in(seed_key, 12), (), 0, device_row_total)
    tallies = jnp.where(jnp.arange(device_row_total, dtype=jnp.int32) == fullest_device, per_device, tallies)
    return jnp.arange(per_device, dtype=jnp.int32)[None, :] < tallies[:, None]


def slot_tallies(seed_key, device_row_total, directions, bound, full_direction, fullest_device):
    tallies = jax.random.randint(jax.random.fold_in(seed_key, 1), (device_row_total, directions), 1, bound + 1)
    marked = jnp.logical_and(jnp.arange(device_row_total, dtype=jnp.int32)[:, None] == fullest_device, jnp.arange(directions, dtype=jnp.int32)[None, :] == full_direction)
    return jnp.where(marked, bound, tallies).astype(jnp.int32)


def adjacent_slot(seed_key, owning_device_ids, directions, lat_table, tallies, bound):
    total = owning_device_ids.shape[0]
    direction = jax.random.randint(jax.random.fold_in(seed_key, 3), (total,), 0, directions)
    lat_step = jnp.array(lat_table, dtype=jnp.int32)[direction]
    source_lat = owning_device_ids // N_LON - lat_step
    within_bounds = jnp.logical_and(source_lat >= 0, source_lat < N_LAT)
    spread = jax.random.randint(jax.random.fold_in(seed_key, 4), (total,), 0, 1 << 20)
    position = spread % tallies[owning_device_ids, direction]
    return ((direction * bound + position).astype(jnp.int32), within_bounds)


def draw_g2m_sender(key, part):
    device_row_total = G2M // E_G2M
    slot_numbers = jnp.arange(G2M, dtype=jnp.int32)
    owning_device_ids = slot_numbers // E_G2M
    fullest_device = jax.random.randint(jax.random.fold_in(key, 401), (), 0, device_row_total)
    tallies = slot_tallies(jax.random.fold_in(key, 402), device_row_total, 4, GSLOT, 3, fullest_device)
    adjacent_index, within_bounds = adjacent_slot(jax.random.fold_in(key, 403), owning_device_ids, 4, GRID_LAT_STEPS, tallies, GSLOT)
    chooser = jax.random.randint(jax.random.fold_in(key, 404), (G2M,), 0, 4)
    own_rows = jax.random.randint(jax.random.fold_in(key, 405), (G2M,), 0, GRID_DEV)
    final_output = jnp.where(jnp.logical_or(chooser < 2, jnp.logical_not(within_bounds)), own_rows, GRID_DEV + adjacent_index)
    starting_slot = fullest_device * E_G2M
    final_output = jnp.where(slot_numbers == starting_slot, GRID_DEV + 4 * GSLOT - 1, final_output)
    final_output = jnp.where(slot_numbers == starting_slot + 1, 0, final_output)
    return final_output.astype(jnp.int32)


def draw_g2m_receiver(key, part):
    device_row_total = G2M // E_G2M
    live_slots = live_mask(jax.random.fold_in(key, 101), device_row_total, E_G2M)
    picked = jax.random.randint(jax.random.fold_in(key, 102), (device_row_total, E_G2M), 0, MESH_PER_DEVICE)
    return jnp.where(live_slots, picked, MESH_PER_DEVICE).reshape(-1).astype(jnp.int32)


def draw_mesh_receiver(key, part):
    device_row_total = MESH_EDGE_SLOTS // E_MESH
    live_slots = live_mask(jax.random.fold_in(key, 201), device_row_total, E_MESH)
    picked = jax.random.randint(jax.random.fold_in(key, 202), (device_row_total, E_MESH), 0, MESH_PER_DEVICE)
    return jnp.where(live_slots, picked, MESH_PER_DEVICE).reshape(-1).astype(jnp.int32)


def draw_mesh_sender(key, part):
    device_row_total = MESH_EDGE_SLOTS // E_MESH
    slot_numbers = jnp.arange(MESH_EDGE_SLOTS, dtype=jnp.int32)
    owning_device_ids = slot_numbers // E_MESH
    fullest_device = jax.random.randint(jax.random.fold_in(key, 301), (), 0, device_row_total)
    tallies = slot_tallies(jax.random.fold_in(key, 302), device_row_total, 8, NEAR_ROW_SLOTS, 4, fullest_device)
    adjacent_index, within_bounds = adjacent_slot(jax.random.fold_in(key, 303), owning_device_ids, 8, MESH_LATITUDES, tallies, NEAR_ROW_SLOTS)
    chooser = jax.random.randint(jax.random.fold_in(key, 304), (MESH_EDGE_SLOTS,), 0, 20)
    own_rows = jax.random.randint(jax.random.fold_in(key, 305), (MESH_EDGE_SLOTS,), 0, MESH_PER_DEVICE)
    far_base = MESH_PER_DEVICE + 8 * NEAR_ROW_SLOTS
    random_source = jax.random.randint(jax.random.fold_in(key, 306), (MESH_EDGE_SLOTS,), 0, device_row_total)
    opposite_source = (owning_device_ids + device_row_total // 2) % device_row_total
    coin = jax.random.randint(jax.random.fold_in(key, 307), (MESH_EDGE_SLOTS,), 0, 2)
    far_source = jnp.where(coin == 0, opposite_source, random_source)
    far_slot = jax.random.randint(jax.random.fold_in(key, 308), (MESH_EDGE_SLOTS,), 0, FAR_ROW_SLOTS)
    distant_rows = far_base + far_source * FAR_ROW_SLOTS + far_slot
    opposite_rows = far_base + opposite_source * FAR_ROW_SLOTS + far_slot
    near_rows = jnp.where(within_bounds, MESH_PER_DEVICE + adjacent_index, own_rows)
    final_output = jnp.where(chooser < 13, own_rows, jnp.where(chooser < 17, near_rows, distant_rows))
    starting_slot = fullest_device * E_MESH
    final_output = jnp.where(slot_numbers == starting_slot, far_base + device_row_total * FAR_ROW_SLOTS - 1, final_output)
    final_output = jnp.where(slot_numbers == starting_slot + 1, 0, final_output)
    final_output = jnp.where(slot_numbers == starting_slot + 2, MESH_PER_DEVICE + 5 * NEAR_ROW_SLOTS - 1, final_output)
    forced = jnp.logical_and(slot_numbers >= starting_slot + 3, slot_numbers < starting_slot + 6)
    final_output = jnp.where(forced, opposite_rows, final_output)
    return final_output.astype(jnp.int32)


def plant(values, stream_key, smallest, largest):
    longest = values.shape.index(max(values.shape))
    spots = []
    for shift in (0, 1):
        where = [jax.random.randint(jax.random.fold_in(stream_key, axis), (), 0, length) for axis, length in enumerate(values.shape)]
        where[longest] = (where[longest] + shift) % values.shape[longest]
        spots.append(tuple(where))
    return values.at[spots[0]].set(smallest).at[spots[1]].set(largest)


def block_scale(own_key, extent, cuts, low, largest):
    factor_of = 1.0
    for dim, shards_of in cuts:
        steps = jax.random.uniform(jax.random.fold_in(jax.random.fold_in(own_key, 6), dim), (shards_of,), jnp.float32, low / len(cuts), largest / len(cuts))
        factor_of = factor_of * jnp.repeat(jnp.exp(steps), extent[dim] // shards_of).reshape((-1,) + (1,) * (len(extent) - 1 - dim))
    return factor_of


def centred(key, shape, width, most, cuts=(), kind=jnp.bfloat16):
    values = jax.random.normal(key, shape, jnp.float32) * width
    if len(cuts) > 0:
        values = block_scale(key, shape, cuts, -0.22, 0.18) * values
    return jnp.clip(values, min=-most, max=most).astype(kind)


def setup_inputs(seed: int = 0) -> dict:
    streams_of = jax.random.split(jax.random.key(seed), 17)
    grid_feat = centred(streams_of[0], (GRID, C_IN), 1.0, 6.0, ((0, 128),))
    grid_send = plant(jax.random.randint(streams_of[1], (DEVICES, 4, GSLOT), 0, GRID_DEV), jax.random.fold_in(streams_of[1], 1), 0, GRID_DEV - 1).astype(jnp.int32)
    g2m_sender = draw_g2m_sender(jax.random.fold_in(streams_of[16], 71), 0)
    g2m_receiver = draw_g2m_receiver(jax.random.fold_in(streams_of[16], 71), 0)
    g2m_geom = jnp.clip(jax.random.uniform(streams_of[4], (4, G2M), jnp.float32, -1.0, 1.0) * block_scale(streams_of[4], (4, G2M), ((1, 128),), -0.4, 0.0), -1.0, 1.0)
    mesh_geom = jnp.clip(jax.random.uniform(streams_of[5], (3, MESH), jnp.float32, -1.0, 1.0) * block_scale(streams_of[5], (3, MESH), ((1, 128),), -0.4, 0.0), -1.0, 1.0)
    mesh_adjacent_lists = plant(jax.random.randint(streams_of[6], (DEVICES, 8, NEAR_ROW_SLOTS), 0, MESH_PER_DEVICE), jax.random.fold_in(streams_of[6], 1), 0, MESH_PER_DEVICE - 1).astype(jnp.int32)
    mesh_far = plant(jax.random.randint(streams_of[7], (DEVICES, DEVICES, FAR_ROW_SLOTS), 0, MESH_PER_DEVICE), jax.random.fold_in(streams_of[7], 1), 0, MESH_PER_DEVICE - 1).astype(jnp.int32)
    mesh_sender = draw_mesh_sender(jax.random.fold_in(streams_of[16], 71), 0)
    mesh_receiver = draw_mesh_receiver(jax.random.fold_in(streams_of[16], 71), 0)
    mesh_edge_geom = jnp.clip(jax.random.uniform(streams_of[10], (4, MESH_EDGE_SLOTS), jnp.float32, -1.0, 1.0) * block_scale(streams_of[10], (4, MESH_EDGE_SLOTS), ((1, 128),), -0.4, 0.0), -1.0, 1.0)
    embed_in = centred(streams_of[11], (C_IN, D), C_IN ** -0.5, 0.25)
    mesh_in = centred(streams_of[12], (3, D), 3 ** -0.5, 3.5, (), jnp.float32)
    geo_in = centred(streams_of[13], (SECTIONS, 4, D), 4 ** -0.5, 3.0, (), jnp.float32)
    pair_in = centred(streams_of[14], (SECTIONS, 4, D, D), (2 * D) ** -0.5, 0.1875)
    square_out = centred(streams_of[15], (SQUARES, D, D), D ** -0.5, 0.25)
    return {"grid_feat": grid_feat, "grid_send": grid_send, "g2m_sender": g2m_sender, "g2m_receiver": g2m_receiver, "g2m_geom": g2m_geom, "mesh_geom": mesh_geom, "mesh_adjacent_lists": mesh_adjacent_lists, "mesh_far": mesh_far, "mesh_sender": mesh_sender, "mesh_receiver": mesh_receiver, "mesh_edge_geom": mesh_edge_geom, "embed_in": embed_in, "mesh_in": mesh_in, "geo_in": geo_in, "pair_in": pair_in, "square_out": square_out}


EPSILON = 1e-05
GRID_OFFSETS = ((-1, 0), (1, 0), (0, -1), (0, 1))
MESH_OFFSETS = ((-1, -1), (-1, 0), (-1, 1), (0, -1), (0, 1), (1, -1), (1, 0), (1, 1))

def layer_norm(values):
    centre = values - lax.optimization_barrier(jnp.mean(values, axis=-1, keepdims=True))
    spread = lax.optimization_barrier(jnp.mean(centre * centre, axis=-1, keepdims=True))
    return centre * lax.rsqrt(spread + EPSILON)

def two_layer(pre_act, out_weight):
    hidden = jax.nn.silu(pre_act).astype(jnp.bfloat16)
    return layer_norm(jnp.dot(hidden, out_weight, preferred_element_type=jnp.float32))

def edge_sums(sender_term, receiver_term, senders, receivers, geometry, geo_weight, out_weight):
    node_count = receiver_term.shape[0]
    row_ids = jnp.minimum(receivers, node_count - 1)
    pre_act = jnp.dot(geometry.T, geo_weight, precision=lax.Precision.HIGHEST)
    pre_act = pre_act + sender_term[senders] + receiver_term[row_ids]
    message = two_layer(pre_act, out_weight).astype(jnp.bfloat16)
    summed = jax.ops.segment_sum(message.astype(jnp.float32), receivers, num_segments=node_count + 1)
    return summed[:node_count]

def node_update(latent, edge_sum, section_weights, out_weight):
    pre_act = jnp.dot(latent, section_weights[2], preferred_element_type=jnp.float32)
    pre_act = pre_act + jnp.dot(edge_sum.astype(jnp.bfloat16), section_weights[3], preferred_element_type=jnp.float32)
    return (latent.astype(jnp.float32) + two_layer(pre_act, out_weight)).astype(jnp.bfloat16)

def neighbour_rows(table, send_lists, device_id, offsets):
    lat_here = device_id // N_LON
    lon_here = device_id % N_LON
    gathered = []
    for offset_id, (lat_step, lon_step) in enumerate(offsets):
        source_lat = lat_here - lat_step
        source_lon = (lon_here - lon_step) % N_LON
        within_bounds = jnp.logical_and(source_lat >= 0, source_lat < N_LAT)
        source_id = (jnp.clip(source_lat, 0, N_LAT - 1) * N_LON + source_lon).astype(jnp.int32)
        rows = table[source_id][send_lists[source_id, offset_id]]
        gathered.append(jnp.where(within_bounds, rows, jnp.zeros_like(rows)))
    return gathered

def reference(grid_feat, grid_send, g2m_sender, g2m_receiver, g2m_geom, mesh_geom, mesh_adjacent_lists, mesh_far, mesh_sender, mesh_receiver, mesh_edge_geom, embed_in, mesh_in, geo_in, pair_in, square_out):
    device_row_total = N_LAT * N_LON
    source = jnp.arange(device_row_total, dtype=jnp.int32)[:, None]
    device_ids = jnp.arange(device_row_total, dtype=jnp.int32)

    def embed_rows(rows_in):
        pre_act = jnp.dot(rows_in, embed_in, preferred_element_type=jnp.float32)
        return two_layer(pre_act, square_out[0]).astype(jnp.bfloat16)
    grid_latent = lax.map(embed_rows, grid_feat.reshape(device_row_total, GRID_DEV, C_IN))

    def encode(inputs):
        device_id, senders, receivers, geometry, node_geo = inputs
        blocks = [grid_latent[device_id]] + neighbour_rows(grid_latent, grid_send, device_id, GRID_OFFSETS)
        received = jnp.concatenate(blocks, axis=0)
        sender_term = jnp.dot(received, pair_in[0, 0], preferred_element_type=jnp.float32)
        mesh_first = jnp.dot(node_geo.T, mesh_in, precision=lax.Precision.HIGHEST)
        mesh_start = two_layer(mesh_first, square_out[1]).astype(jnp.bfloat16)
        receiver_term = jnp.dot(mesh_start, pair_in[0, 1], preferred_element_type=jnp.float32)
        edge_sum = edge_sums(sender_term, receiver_term, senders, receivers, geometry, geo_in[0], square_out[2])
        return node_update(mesh_start, edge_sum, pair_in[0], square_out[3])
    mesh_latent = lax.map(encode, (device_ids, g2m_sender.reshape(device_row_total, E_G2M), g2m_receiver.reshape(device_row_total, E_G2M), g2m_geom.reshape(4, device_row_total, E_G2M).transpose(1, 0, 2), mesh_geom.reshape(3, device_row_total, MESH_PER_DEVICE).transpose(1, 0, 2)))
    edge_senders = mesh_sender.reshape(device_row_total, E_MESH)
    edge_receivers = mesh_receiver.reshape(device_row_total, E_MESH)
    edge_geometry = mesh_edge_geom.reshape(4, device_row_total, E_MESH).transpose(1, 0, 2)
    for section_id in range(1, STEPS + 1):

        def process(inputs, section_id=section_id, previous=mesh_latent):
            device_id, senders, receivers, geometry = inputs
            own_rows = previous[device_id]
            near_blocks = neighbour_rows(previous, mesh_adjacent_lists, device_id, MESH_OFFSETS)
            far_block = previous[source, mesh_far[:, device_id, :]].reshape(-1, D)
            sender_table = jnp.concatenate([own_rows] + near_blocks + [far_block], axis=0)
            sender_term = jnp.dot(sender_table, pair_in[section_id, 0], preferred_element_type=jnp.float32)
            receiver_term = jnp.dot(own_rows, pair_in[section_id, 1], preferred_element_type=jnp.float32)
            edge_sum = edge_sums(sender_term, receiver_term, senders, receivers, geometry, geo_in[section_id], square_out[2 + 2 * section_id])
            return node_update(own_rows, edge_sum, pair_in[section_id], square_out[3 + 2 * section_id])
        mesh_latent = lax.map(process, (device_ids, edge_senders, edge_receivers, edge_geometry))
    return mesh_latent.reshape(MESH, D)
```

```python
import jax
import jax.numpy as jnp
from jax import lax
from jax.experimental import pallas as pl
from jax.experimental.pallas import tpu as pltpu
from jax.sharding import PartitionSpec as P

EPSILON = 1e-05
GRID_OFFSETS = ((-1, 0), (1, 0), (0, -1), (0, 1))
MESH_OFFSETS = ((-1, -1), (-1, 0), (-1, 1), (0, -1), (0, 1), (1, -1), (1, 0), (1, 1))
N_LAT, N_LON = 16, 8
DEVICES = N_LAT * N_LON
D = 512
LANES = 128
PARTS = D // LANES
C_IN = 474
GRID_DEV = 1024
GSLOT = 256
NODES = 320
NEAR = 112
FAR = 4
EDGES = 4096
CHUNK = 512
KX = NODES + 16
NEAR_ROWS = 8 * NEAR
MESH_AXES = pl.DeviceIdType.MESH
BF16, F32 = jnp.bfloat16, jnp.float32


def matmul(left, right):
    return jnp.dot(left, right, preferred_element_type=F32)


def silu(x):
    half = 0.5 * x
    return half * jnp.tanh(half) + half


def layer_norm(values):
    centre = values - jnp.sum(values, axis=-1, keepdims=True) * (1.0 / D)
    spread = jnp.sum(centre * centre, axis=-1, keepdims=True) * (1.0 / D)
    return centre * lax.rsqrt(spread + EPSILON)


def split_high_low(values):
    high = values.astype(BF16).astype(F32)
    return high, (values - high).astype(BF16).astype(F32)


def store_rows(table, first, values):
    rows = values.shape[0]
    for part in range(PARTS):
        table[pl.ds(first * PARTS + part, rows, stride=PARTS), :] = values[
            :, part * LANES : (part + 1) * LANES
        ]


def load_rows(table, first, rows):
    return jnp.concatenate(
        [table[pl.ds(first * PARTS + part, rows, stride=PARTS), :] for part in range(PARTS)],
        axis=1,
    )


def kernel(
    grid_send, g2m_sender, near_lists, far_lists, mesh_sender,
    g2m_receiver, g2m_geom, mesh_geom, mesh_receiver, mesh_edge_geom, mesh_in, geo_in,
    grid_hbm, embed_hbm, pair_hbm, square_hbm,
    out,
    grid, embed, pair, square,
    table, staged, grid_out, grid_arrived, near_out, near_arrived, far_out, far_arrived,
    geo_x, geo_w, x_grid, x_mesh, y_rows, pre, gathered, hidden, edge_sum, latent,
    load_sem, grid_ssem, grid_rsem, near_ssem, near_rsem, far_ssem, far_rsem,
):
    lat = lax.axis_index("lat")
    lon = lax.axis_index("lon")
    me = lat * N_LON + lon

    loads = [
        pltpu.make_async_copy(grid_hbm, grid, load_sem.at[0]),
        pltpu.make_async_copy(embed_hbm, embed, load_sem.at[1]),
        pltpu.make_async_copy(square_hbm, square, load_sem.at[2]),
        pltpu.make_async_copy(pair_hbm, pair, load_sem.at[3]),
    ]
    for load in loads:
        load.start()

    barrier = pltpu.get_barrier_semaphore()

    def greet(step, carry):
        other = lax.rem(me + step, DEVICES)
        pl.semaphore_signal(
            barrier, inc=1, device_id=(other // N_LON, lax.rem(other, N_LON)),
            device_id_type=MESH_AXES,
        )
        return carry

    lax.fori_loop(1, DEVICES, greet, 0)

    def send_to(offset, source, target, ssem, rsem):
        lat_step, lon_step = offset
        there = lat + lat_step
        copy = pltpu.make_async_remote_copy(
            source, target, ssem, rsem,
            device_id=(there, lax.rem(lon + lon_step + N_LON, N_LON)),
            device_id_type=MESH_AXES,
        )
        return copy, jnp.logical_and(there >= 0, there < N_LAT)

    def source_exists(offset):
        here = lat - offset[0]
        return jnp.logical_and(here >= 0, here < N_LAT)

    for load in loads:
        load.wait()
    rows_at_once = 256

    def embed_rows(block, carry):
        rows = pl.ds(pl.multiple_of(block * rows_at_once, rows_at_once), rows_at_once)
        first = silu(matmul(grid[rows, :], embed[...])).astype(BF16)
        grid_latent = layer_norm(matmul(first, square[0])).astype(BF16)
        store_rows(table, block * rows_at_once, matmul(grid_latent, pair[0, 0]))
        return carry

    lax.fori_loop(0, GRID_DEV // rows_at_once, embed_rows, 0)

    def pick(list_ref, first_of, count):
        def some(block, carry):
            for k in range(16):
                slot = block * 16 + k
                row = list_ref(slot)
                staged[pl.ds(pl.multiple_of((first_of + slot) * PARTS, PARTS), PARTS), :] = table[
                    pl.ds(row * PARTS, PARTS), :
                ]
            return carry
        lax.fori_loop(0, count // 16, some, 0)

    def run_if(condition, offset, act):
        if offset[0] == 0:
            act()
        else:
            pl.when(condition)(act)

    pl.semaphore_wait(barrier, DEVICES - 1)
    grid_sends = []
    for d, offset in enumerate(GRID_OFFSETS):
        pick(lambda slot, d=d: grid_send[0, d, slot], d * GSLOT, GSLOT)
        grid_out[d] = staged[pl.ds(d * GSLOT * PARTS, GSLOT * PARTS), :].astype(BF16)
        copy, exists = send_to(
            offset, grid_out.at[d], grid_arrived.at[d], grid_ssem.at[d], grid_rsem.at[d]
        )
        run_if(exists, offset, copy.start)
        grid_sends.append((copy, exists, offset))

    def build_x(x_ref, receiver, geometry):
        high, low = split_high_low(geometry[...])
        geo_x[0:4, :] = high
        geo_x[4:8, :] = low
        geo_x[8:12, :] = high
        geo_x[12:16, :] = jnp.zeros((4, EDGES), F32)
        x_ref[NODES:KX, :] = geo_x[...].astype(BF16)

        def some(block, carry):
            columns = pl.ds(pl.multiple_of(block * CHUNK, CHUNK), CHUNK)
            node = lax.broadcasted_iota(jnp.int32, (NODES, CHUNK), 0)
            x_ref[0:NODES, columns] = jnp.where(node == receiver[:, columns], 1.0, 0.0).astype(BF16)
            return carry

        lax.fori_loop(0, EDGES // CHUNK, some, 0)

    def pre_activation(section, x_ref):
        y_rows[0:NODES, :] = matmul(latent[...], pair[section, 1]).astype(BF16)
        high, low = split_high_low(geo_in[section])
        geo_w[0:4, :] = high
        geo_w[4:8, :] = high
        geo_w[8:12, :] = low
        geo_w[12:16, :] = jnp.zeros((4, D), F32)
        y_rows[NODES:KX, :] = geo_w[...].astype(BF16)

        def some(block, carry):
            chunk = pl.ds(pl.multiple_of(block * CHUNK, CHUNK), CHUNK)
            pre[chunk, :] = lax.dot_general(
                x_ref[:, chunk], y_rows[...], (((0,), (0,)), ((), ())), preferred_element_type=F32
            )
            return carry

        lax.fori_loop(0, EDGES // CHUNK, some, 0)

    build_x(x_grid, g2m_receiver, g2m_geom)
    high, low = split_high_low(mesh_geom[...])
    geo_x[0:3, 0:NODES] = high
    geo_x[3:6, 0:NODES] = low
    geo_x[6:9, 0:NODES] = high
    geo_x[9:16, 0:NODES] = jnp.zeros((7, NODES), F32)
    high, low = split_high_low(mesh_in[...])
    geo_w[0:3, :] = high
    geo_w[3:6, :] = high
    geo_w[6:9, :] = low
    geo_w[9:16, :] = jnp.zeros((7, D), F32)
    mesh_first = lax.dot_general(
        geo_x[:, 0:NODES].astype(BF16), geo_w[...].astype(BF16), (((0,), (0,)), ((), ())),
        preferred_element_type=F32,
    )
    latent[...] = layer_norm(matmul(silu(mesh_first).astype(BF16), square[1])).astype(BF16)
    pre_activation(0, x_grid)
    build_x(x_mesh, mesh_receiver, mesh_edge_geom)

    def edges(section, senders, x_ref):
        edge_sum[...] = jnp.zeros((NODES, D), F32)

        def some(block, carry):
            base = block * CHUNK
            chunk = pl.ds(pl.multiple_of(base, CHUNK), CHUNK)

            def gather(group, inner):
                for k in range(32):
                    slot = group * 32 + k
                    row = senders[base + slot]
                    gathered[pl.ds(pl.multiple_of(slot * PARTS, PARTS), PARTS), :] = table[
                        pl.ds(row * PARTS, PARTS), :
                    ]
                return inner

            lax.fori_loop(0, CHUNK // 32, gather, 0)
            hidden[...] = silu(pre[chunk, :] + load_rows(gathered, 0, CHUNK)).astype(BF16)
            message = layer_norm(matmul(hidden[...], square[2 + 2 * section])).astype(BF16)
            edge_sum[...] += matmul(x_ref[0:NODES, chunk], message)
            return carry

        lax.fori_loop(0, EDGES // CHUNK, some, 0)

    def node_update(section):
        before = latent[...]
        first = matmul(before, pair[section, 2]) + matmul(
            edge_sum[...].astype(BF16), pair[section, 3]
        )
        second = layer_norm(matmul(silu(first).astype(BF16), square[3 + 2 * section]))
        return (before.astype(F32) + second).astype(BF16)

    for d, offset in enumerate(GRID_OFFSETS):
        copy = grid_sends[d][0]
        run_if(source_exists(offset), offset, copy.wait_recv)
        table[pl.ds((GRID_DEV + d * GSLOT) * PARTS, GSLOT * PARTS), :] = grid_arrived[d].astype(F32)
    edges(0, g2m_sender, x_grid)
    latent[...] = node_update(0)

    all_sends = list(grid_sends)
    far_waits = []
    for section in (1, 2):
        step = section - 1
        store_rows(table, 0, matmul(latent[...], pair[section, 0]))
        for d in (0, 1, 2, 5, 6, 7, 3, 4):
            offset = MESH_OFFSETS[d]
            pick(lambda slot, d=d: near_lists[0, d, slot], 0, NEAR)
            near_out[step, d] = staged[0 : NEAR * PARTS, :].astype(BF16)
            copy, exists = send_to(
                offset, near_out.at[step, d], near_arrived.at[step, d],
                near_ssem.at[step, d], near_rsem.at[step, d],
            )
            run_if(exists, offset, copy.start)
            all_sends.append((copy, exists, offset))
        pick(lambda slot: far_lists[0, slot // FAR, lax.rem(slot, FAR)], 0, DEVICES * FAR)
        far_out[step] = staged[0 : DEVICES * FAR * PARTS, :].astype(BF16).reshape(
            DEVICES, FAR * PARTS, LANES
        )
        far_arrived[step, me] = far_out[step, me]

        def send_far(k, carry, step=step):
            other = lax.rem(me + k, DEVICES)
            pltpu.make_async_remote_copy(
                far_out.at[step, other], far_arrived.at[step, me],
                far_ssem.at[step], far_rsem.at[step],
                device_id=(other // N_LON, lax.rem(other, N_LON)), device_id_type=MESH_AXES,
            ).start()
            return carry

        lax.fori_loop(1, DEVICES, send_far, 0)
        pre_activation(section, x_mesh)

        for d, offset in enumerate(MESH_OFFSETS):
            copy, exists = send_to(
                offset, near_out.at[step, d], near_arrived.at[step, d],
                near_ssem.at[step, d], near_rsem.at[step, d],
            )
            run_if(source_exists(offset), offset, copy.wait_recv)
            table[pl.ds((NODES + d * NEAR) * PARTS, NEAR * PARTS), :] = near_arrived[step, d].astype(F32)
        far_wait = pltpu.make_async_remote_copy(
            far_out.at[step, pl.ds(0, DEVICES - 1)], far_arrived.at[step, pl.ds(0, DEVICES - 1)],
            far_ssem.at[step], far_rsem.at[step],
            device_id=(lat, lax.rem(lon + 1, N_LON)), device_id_type=MESH_AXES,
        )
        far_wait.wait_recv()
        far_waits.append(far_wait)
        table[pl.ds((NODES + NEAR_ROWS) * PARTS, DEVICES * FAR * PARTS), :] = far_arrived[step].astype(
            F32
        ).reshape(DEVICES * FAR * PARTS, LANES)
        edges(section, mesh_sender, x_mesh)
        latent[...] = node_update(section)

    out[...] = latent[...]
    for copy, exists, offset in all_sends:
        run_if(exists, offset, copy.wait_send)
    for far_wait in far_waits:
        far_wait.wait_send()


def per_device(
    grid_feat, grid_send, g2m_sender, g2m_receiver, g2m_geom, mesh_geom, mesh_adjacent_lists,
    mesh_far, mesh_sender, mesh_receiver, mesh_edge_geom, embed_in, mesh_in, geo_in, pair_in,
    square_out,
):
    smem = pl.BlockSpec(memory_space=pltpu.SMEM)
    vmem = pl.BlockSpec(memory_space=pltpu.VMEM)
    hbm = pl.BlockSpec(memory_space=pl.ANY)
    dma = pltpu.SemaphoreType.DMA
    return pl.pallas_call(
        kernel,
        out_shape=jax.ShapeDtypeStruct((NODES, D), BF16),
        in_specs=[smem] * 5 + [vmem] * 7 + [hbm] * 4,
        out_specs=vmem,
        scratch_shapes=[
            pltpu.VMEM((GRID_DEV, C_IN), BF16),
            pltpu.VMEM((C_IN, D), BF16),
            pltpu.VMEM((3, 4, D, D), BF16),
            pltpu.VMEM((8, D, D), BF16),
            pltpu.VMEM(((GRID_DEV + 4 * GSLOT) * PARTS, LANES), F32),
            pltpu.VMEM((4 * GSLOT * PARTS, LANES), F32),
            pltpu.VMEM((4, GSLOT * PARTS, LANES), BF16),
            pltpu.VMEM((4, GSLOT * PARTS, LANES), BF16),
            pltpu.VMEM((2, 8, NEAR * PARTS, LANES), BF16),
            pltpu.VMEM((2, 8, NEAR * PARTS, LANES), BF16),
            pltpu.VMEM((2, DEVICES, FAR * PARTS, LANES), BF16),
            pltpu.VMEM((2, DEVICES, FAR * PARTS, LANES), BF16),
            pltpu.VMEM((16, EDGES), F32),
            pltpu.VMEM((16, D), F32),
            pltpu.VMEM((KX, EDGES), BF16),
            pltpu.VMEM((KX, EDGES), BF16),
            pltpu.VMEM((KX, D), BF16),
            pltpu.VMEM((EDGES, D), F32),
            pltpu.VMEM((CHUNK * PARTS, LANES), F32),
            pltpu.VMEM((CHUNK, D), BF16),
            pltpu.VMEM((NODES, D), F32),
            pltpu.VMEM((NODES, D), BF16),
            dma((4,)), dma((4,)), dma((4,)), dma((2, 8)), dma((2, 8)), dma((2,)), dma((2,)),
        ],
        compiler_params=pltpu.CompilerParams(
            collective_id=0, has_side_effects=True, vmem_limit_bytes=62 * 1024 * 1024
        ),
        name="encoder_processor",
    )(
        grid_send, g2m_sender, mesh_adjacent_lists, mesh_far, mesh_sender,
        g2m_receiver.reshape(1, EDGES), g2m_geom, mesh_geom, mesh_receiver.reshape(1, EDGES),
        mesh_edge_geom, mesh_in, geo_in,
        grid_feat, embed_in, pair_in, square_out,
    )


def solution(mesh):
    split = ("lat", "lon")
    in_specs = (
        P(split, None), P(split, None, None), P(split), P(split), P(None, split), P(None, split),
        P(split, None, None), P(split, None, None), P(split), P(split), P(None, split),
        P(), P(), P(), P(), P(),
    )
    return jax.shard_map(
        per_device, mesh=mesh, in_specs=in_specs, out_specs=P(split, None), check_vma=False
    )
```

```python
import jax
import jax.numpy as jnp
from jax import lax
from jax.experimental import pallas as pl
from jax.experimental.pallas import tpu as pltpu
from jax.sharding import PartitionSpec as P

EPSILON = 1e-05
GRID_OFFSETS = ((-1, 0), (1, 0), (0, -1), (0, 1))
MESH_OFFSETS = ((-1, -1), (-1, 0), (-1, 1), (0, -1), (0, 1), (1, -1), (1, 0), (1, 1))
N_LAT, N_LON = 16, 8
DEVICES = N_LAT * N_LON
D = 512
LANES = 128
PARTS = D // LANES
C_IN = 474
GRID_DEV = 1024
GSLOT = 256
NODES = 320
NEAR = 112
FAR = 4
EDGES = 4096
CHUNK = 512
HALF = CHUNK // 2
SLICE = 64
KX = NODES + 16
NEAR_ROWS = 8 * NEAR
MESH_AXES = pl.DeviceIdType.MESH
BF16, F32 = jnp.bfloat16, jnp.float32


def matmul(left, right):
    return jnp.dot(left, right, preferred_element_type=F32)


def silu_of_half(half):
    return half * jnp.tanh(half) + half


def silu(x):
    return silu_of_half(0.5 * x)


def layer_norm(values):
    centre = values - jnp.sum(values, axis=-1, keepdims=True) * (1.0 / D)
    spread = jnp.sum(centre * centre, axis=-1, keepdims=True) * (1.0 / D)
    return centre * lax.rsqrt(spread + EPSILON)


def split_high_low(values):
    high = values.astype(BF16).astype(F32)
    return high, (values - high).astype(BF16).astype(F32)


def store_rows(table, first, values):
    rows = values.shape[0]
    for part in range(PARTS):
        table[pl.ds(first * PARTS + part, rows, stride=PARTS), :] = values[
            :, part * LANES : (part + 1) * LANES
        ]


def load_rows(table, first, rows):
    return jnp.concatenate(
        [table[pl.ds(first * PARTS + part, rows, stride=PARTS), :] for part in range(PARTS)],
        axis=1,
    )


def kernel(
    grid_send, g2m_sender, near_lists, far_lists, mesh_sender,
    g2m_receiver, g2m_geom, mesh_geom, mesh_receiver, mesh_edge_geom, mesh_in, geo_in,
    grid_hbm, embed_hbm, pair_hbm, square_hbm,
    out,
    grid, embed, pair, square,
    table, staged, grid_out, grid_arrived, near_out, near_arrived, far_out, far_arrived,
    geo_x, geo_w, x_grid, x_mesh, y_rows, pre, gathered_0, gathered_1, hidden_0, hidden_1, product_0, product_1, message_0, message_1,
    edge_sum, latent,
    load_sem, grid_ssem, grid_rsem, near_ssem, near_rsem, far_ssem, far_rsem,
):
    lat = lax.axis_index("lat")
    lon = lax.axis_index("lon")
    me = lat * N_LON + lon
    lats = [lax.rem(lat + step, N_LAT) for step in range(N_LAT)]
    lons = [lax.rem(lon + step, N_LON) for step in range(N_LON)]
    others = [(a, b) for a in range(N_LAT) for b in range(N_LON) if a or b]
    gathered, hidden = (gathered_0, gathered_1), (hidden_0, hidden_1)
    product, message = (product_0, product_1), (message_0, message_1)

    loads = [
        pltpu.make_async_copy(source, target, load_sem.at[k])
        for k, (source, target) in enumerate((
            (grid_hbm, grid), (embed_hbm, embed),
            (square_hbm.at[0], square.at[0]), (pair_hbm.at[0, 0], pair.at[0, 0]),
            (square_hbm.at[pl.ds(1, 7)], square.at[pl.ds(1, 7)]),
            (pair_hbm.at[0, pl.ds(1, 3)], pair.at[0, pl.ds(1, 3)]),
            (pair_hbm.at[pl.ds(1, 2)], pair.at[pl.ds(1, 2)]),
        ))
    ]
    for load in loads:
        load.start()

    barrier = pltpu.get_barrier_semaphore()

    for a, b in others:
        pl.semaphore_signal(
            barrier, inc=1, device_id=(lats[a], lons[b]), device_id_type=MESH_AXES
        )

    def send_to(offset, source, target, ssem, rsem):
        lat_step, lon_step = offset
        there = lat + lat_step
        copy = pltpu.make_async_remote_copy(
            source, target, ssem, rsem,
            device_id=(there, lax.rem(lon + lon_step + N_LON, N_LON)),
            device_id_type=MESH_AXES,
        )
        return copy, jnp.logical_and(there >= 0, there < N_LAT)

    def source_exists(offset):
        here = lat - offset[0]
        return jnp.logical_and(here >= 0, here < N_LAT)

    for load in loads[:4]:
        load.wait()
    rows_at_once = 256

    def embed_rows(block, carry):
        rows = pl.ds(pl.multiple_of(block * rows_at_once, rows_at_once), rows_at_once)
        first = lax.dot_general(
            grid[:, rows], embed[...], (((0,), (0,)), ((), ())), preferred_element_type=F32
        )
        first = silu(first).astype(BF16)
        grid_latent = layer_norm(matmul(first, square[0])).astype(BF16)
        store_rows(table, block * rows_at_once, 0.5 * matmul(grid_latent, pair[0, 0]))
        return carry

    lax.fori_loop(0, GRID_DEV // rows_at_once, embed_rows, 0)

    def copy_row(target, slot, row):
        target[pl.ds(slot * PARTS, PARTS), :] = table[pl.ds(row * PARTS, PARTS), :]

    def pick(row_of, first, count):
        for k in range(count):
            copy_row(staged, first + k, row_of(k))

    def run_if(condition, offset, act):
        if offset[0] == 0:
            act()
        else:
            pl.when(condition)(act)

    pl.semaphore_wait(barrier, DEVICES - 1)
    grid_sends = []
    for d, offset in enumerate(GRID_OFFSETS):
        pick(lambda slot, d=d: grid_send[0, d, slot], d * GSLOT, GSLOT)
        grid_out[d] = staged[pl.ds(d * GSLOT * PARTS, GSLOT * PARTS), :].astype(BF16)
        copy, exists = send_to(
            offset, grid_out.at[d], grid_arrived.at[d], grid_ssem.at[d], grid_rsem.at[d]
        )
        run_if(exists, offset, copy.start)
        grid_sends.append((copy, exists, offset))

    def build_x(x_ref, receiver, geometry):
        high, low = split_high_low(geometry[...])
        geo_x[0:4, :] = high
        geo_x[4:8, :] = low
        geo_x[8:12, :] = high
        geo_x[12:16, :] = jnp.zeros((4, EDGES), F32)
        x_ref[NODES:KX, :] = geo_x[...].astype(BF16)

        def some(block, carry):
            columns = pl.ds(pl.multiple_of(block * CHUNK, CHUNK), CHUNK)
            node = lax.broadcasted_iota(jnp.int32, (NODES, CHUNK), 0)
            x_ref[0:NODES, columns] = jnp.where(node == receiver[:, columns], 1.0, 0.0).astype(BF16)
            return carry

        lax.fori_loop(0, EDGES // CHUNK, some, 0)

    def pre_activation(section, x_ref):
        y_rows[0:NODES, :] = (0.5 * matmul(latent[...], pair[section, 1])).astype(BF16)
        high, low = split_high_low(0.5 * geo_in[section])
        geo_w[0:4, :] = high
        geo_w[4:8, :] = high
        geo_w[8:12, :] = low
        geo_w[12:16, :] = jnp.zeros((4, D), F32)
        y_rows[NODES:KX, :] = geo_w[...].astype(BF16)

        def some(block, carry):
            chunk = pl.ds(pl.multiple_of(block * CHUNK, CHUNK), CHUNK)
            pre[chunk, :] = lax.dot_general(
                x_ref[:, chunk], y_rows[...], (((0,), (0,)), ((), ())), preferred_element_type=F32
            )
            return carry

        lax.fori_loop(0, EDGES // CHUNK, some, 0)

    for load in loads[4:]:
        load.wait()
    build_x(x_grid, g2m_receiver, g2m_geom)
    high, low = split_high_low(mesh_geom[...])
    geo_x[0:3, 0:NODES] = high
    geo_x[3:6, 0:NODES] = low
    geo_x[6:9, 0:NODES] = high
    geo_x[9:16, 0:NODES] = jnp.zeros((7, NODES), F32)
    high, low = split_high_low(mesh_in[...])
    geo_w[0:3, :] = high
    geo_w[3:6, :] = high
    geo_w[6:9, :] = low
    geo_w[9:16, :] = jnp.zeros((7, D), F32)
    mesh_first = lax.dot_general(
        geo_x[:, 0:NODES].astype(BF16), geo_w[...].astype(BF16), (((0,), (0,)), ((), ())),
        preferred_element_type=F32,
    )
    latent[...] = layer_norm(matmul(silu(mesh_first).astype(BF16), square[1])).astype(BF16)
    pre_activation(0, x_grid)

    def edges(section, senders, x_ref):
        chunks = EDGES // CHUNK
        edge_sum[...] = jnp.zeros((NODES, D), F32)

        def gather(block, first, count):
            for slot in range(first, first + count):
                copy_row(gathered[block % 2], slot, senders[block * CHUNK + slot])

        def hide(block, first):
            half = pre[pl.ds(block * CHUNK + first, SLICE), :] + load_rows(
                gathered[block % 2], first, SLICE
            )
            hidden[block % 2][first : first + SLICE, :] = silu_of_half(half).astype(BF16)

        def multiply(block, first, count):
            product[block % 2][first : first + count, :] = matmul(
                hidden[block % 2][first : first + count, :], square[2 + 2 * section]
            )

        def normalize(block, first):
            message[block % 2][first : first + SLICE, :] = layer_norm(
                product[block % 2][first : first + SLICE, :]
            ).astype(BF16)

        def add_up(block):
            edge_sum[...] += matmul(
                x_ref[0:NODES, block * CHUNK : (block + 1) * CHUNK], message[block % 2][...]
            )

        gather(0, 0, CHUNK)
        for block in range(chunks + 1):
            for first in range(0, CHUNK, SLICE):
                if block + 1 < chunks:
                    gather(block + 1, first, SLICE)
                if block < chunks:
                    hide(block, first)
                if block >= 1:
                    normalize(block - 1, first)
                if block < chunks and (first + SLICE) % HALF == 0:
                    multiply(block, first + SLICE - HALF, HALF)
            if block >= 1:
                add_up(block - 1)

    def node_update(section):
        before = latent[...]
        first = matmul(before, pair[section, 2]) + matmul(
            edge_sum[...].astype(BF16), pair[section, 3]
        )
        second = layer_norm(matmul(silu(first).astype(BF16), square[3 + 2 * section]))
        return (before.astype(F32) + second).astype(BF16)

    for d, offset in enumerate(GRID_OFFSETS):
        copy = grid_sends[d][0]
        run_if(source_exists(offset), offset, copy.wait_recv)
        table[pl.ds((GRID_DEV + d * GSLOT) * PARTS, GSLOT * PARTS), :] = grid_arrived[d].astype(F32)
    edges(0, g2m_sender, x_grid)
    latent[...] = node_update(0)

    all_sends = list(grid_sends)
    far_waits = []
    for section in (1, 2):
        step = section - 1
        store_rows(table, 0, 0.5 * matmul(latent[...], pair[section, 0]))
        def send_far(step=step):
            for a, b in others:
                pltpu.make_async_remote_copy(
                    far_out.at[step, lats[a] * N_LON + lons[b]], far_arrived.at[step, me],
                    far_ssem.at[step], far_rsem.at[step],
                    device_id=(lats[a], lons[b]), device_id_type=MESH_AXES,
                ).start()

        pick(lambda slot: far_lists[0, slot % FAR, slot // FAR], 0, DEVICES * FAR)
        far_out[step] = staged[0 : DEVICES * FAR * PARTS, :].astype(BF16).reshape(
            DEVICES, FAR * PARTS, LANES
        )
        far_arrived[step, me] = far_out[step, me]
        order = (0, 1, 2, 5, 6, 7, 3, 4)
        for n, d in enumerate(order):
            pick(lambda slot, d=d: near_lists[0, d, slot], n * NEAR, NEAR)
            near_out[step, d] = staged[n * NEAR * PARTS : (n + 1) * NEAR * PARTS, :].astype(BF16)
            if n == 0:
                send_far()
            offset = MESH_OFFSETS[d]
            copy, exists = send_to(
                offset, near_out.at[step, d], near_arrived.at[step, d],
                near_ssem.at[step, d], near_rsem.at[step, d],
            )
            run_if(exists, offset, copy.start)
            all_sends.append((copy, exists, offset))
        if section == 1:
            build_x(x_mesh, mesh_receiver, mesh_edge_geom)
        pre_activation(section, x_mesh)

        for d, offset in enumerate(MESH_OFFSETS):
            copy, exists = send_to(
                offset, near_out.at[step, d], near_arrived.at[step, d],
                near_ssem.at[step, d], near_rsem.at[step, d],
            )
            run_if(source_exists(offset), offset, copy.wait_recv)
            table[pl.ds((NODES + d * NEAR) * PARTS, NEAR * PARTS), :] = near_arrived[step, d].astype(F32)
        far_wait = pltpu.make_async_remote_copy(
            far_out.at[step, pl.ds(0, DEVICES - 1)], far_arrived.at[step, pl.ds(0, DEVICES - 1)],
            far_ssem.at[step], far_rsem.at[step],
            device_id=(lat, lax.rem(lon + 1, N_LON)), device_id_type=MESH_AXES,
        )
        far_wait.wait_recv()
        far_waits.append(far_wait)
        table[pl.ds((NODES + NEAR_ROWS) * PARTS, DEVICES * FAR * PARTS), :] = far_arrived[step].astype(
            F32
        ).reshape(DEVICES * FAR * PARTS, LANES)
        edges(section, mesh_sender, x_mesh)
        latent[...] = node_update(section)

    out[...] = latent[...]
    for copy, exists, offset in all_sends:
        run_if(exists, offset, copy.wait_send)
    for far_wait in far_waits:
        far_wait.wait_send()


def per_device(
    grid_feat, grid_send, g2m_sender, g2m_receiver, g2m_geom, mesh_geom, mesh_adjacent_lists,
    mesh_far, mesh_sender, mesh_receiver, mesh_edge_geom, embed_in, mesh_in, geo_in, pair_in,
    square_out,
):
    smem = pl.BlockSpec(memory_space=pltpu.SMEM)
    vmem = pl.BlockSpec(memory_space=pltpu.VMEM)
    hbm = pl.BlockSpec(memory_space=pl.ANY)
    dma = pltpu.SemaphoreType.DMA
    return pl.pallas_call(
        kernel,
        out_shape=jax.ShapeDtypeStruct((NODES, D), BF16),
        in_specs=[smem] * 5 + [vmem] * 7 + [hbm] * 4,
        out_specs=vmem,
        scratch_shapes=[
            pltpu.VMEM((C_IN, GRID_DEV), BF16),
            pltpu.VMEM((C_IN, D), BF16),
            pltpu.VMEM((3, 4, D, D), BF16),
            pltpu.VMEM((8, D, D), BF16),
            pltpu.VMEM(((GRID_DEV + 4 * GSLOT) * PARTS, LANES), F32),
            pltpu.VMEM((4 * GSLOT * PARTS, LANES), F32),
            pltpu.VMEM((4, GSLOT * PARTS, LANES), BF16),
            pltpu.VMEM((4, GSLOT * PARTS, LANES), BF16),
            pltpu.VMEM((2, 8, NEAR * PARTS, LANES), BF16),
            pltpu.VMEM((2, 8, NEAR * PARTS, LANES), BF16),
            pltpu.VMEM((2, DEVICES, FAR * PARTS, LANES), BF16),
            pltpu.VMEM((2, DEVICES, FAR * PARTS, LANES), BF16),
            pltpu.VMEM((16, EDGES), F32),
            pltpu.VMEM((16, D), F32),
            pltpu.VMEM((KX, EDGES), BF16),
            pltpu.VMEM((KX, EDGES), BF16),
            pltpu.VMEM((KX, D), BF16),
            pltpu.VMEM((EDGES, D), F32),
            pltpu.VMEM((CHUNK * PARTS, LANES), F32), pltpu.VMEM((CHUNK * PARTS, LANES), F32),
            pltpu.VMEM((CHUNK, D), BF16), pltpu.VMEM((CHUNK, D), BF16),
            pltpu.VMEM((CHUNK, D), F32), pltpu.VMEM((CHUNK, D), F32),
            pltpu.VMEM((CHUNK, D), BF16), pltpu.VMEM((CHUNK, D), BF16),
            pltpu.VMEM((NODES, D), F32),
            pltpu.VMEM((NODES, D), BF16),
            dma((7,)), dma((4,)), dma((4,)), dma((2, 8)), dma((2, 8)), dma((2,)), dma((2,)),
        ],
        compiler_params=pltpu.CompilerParams(
            collective_id=0, has_side_effects=True, vmem_limit_bytes=62 * 1024 * 1024
        ),
        name="encoder_processor",
    )(
        grid_send, g2m_sender, mesh_adjacent_lists, jnp.swapaxes(mesh_far, 1, 2), mesh_sender,
        g2m_receiver.reshape(1, EDGES), g2m_geom, mesh_geom, mesh_receiver.reshape(1, EDGES),
        mesh_edge_geom, mesh_in, geo_in,
        grid_feat.T, embed_in, pair_in, square_out,
    )


def solution(mesh):
    split = ("lat", "lon")
    in_specs = (
        P(split, None), P(split, None, None), P(split), P(split), P(None, split), P(None, split),
        P(split, None, None), P(split, None, None), P(split), P(split), P(None, split),
        P(), P(), P(), P(), P(),
    )
    return jax.shard_map(
        per_device, mesh=mesh, in_specs=in_specs, out_specs=P(split, None), check_vma=False
    )
```

```python
import jax
import jax.numpy as jnp
from jax import lax
from jax.experimental import pallas as pl
from jax.experimental.pallas import tpu as pltpu
from jax.sharding import PartitionSpec as P

EPSILON = 1e-05
GRID_OFFSETS = ((-1, 0), (1, 0), (0, -1), (0, 1))
MESH_OFFSETS = ((-1, -1), (-1, 0), (-1, 1), (0, -1), (0, 1), (1, -1), (1, 0), (1, 1))
N_LAT, N_LON = 16, 8
DEVICES = N_LAT * N_LON
D = 512
LANES = 128
PARTS = D // LANES
C_IN = 474
GRID_DEV = 1024
GSLOT = 256
NODES = 320
NEAR = 112
FAR = 4
EDGES = 4096
CHUNK = 512
HALF = CHUNK // 2
SLICE = 32
KX = NODES + 16
NEAR_ROWS = 8 * NEAR
MESH_AXES = pl.DeviceIdType.MESH
BF16, F32 = jnp.bfloat16, jnp.float32


def matmul(left, right):
    return jnp.dot(left, right, preferred_element_type=F32)


def silu_of_half(half):
    return half * jnp.tanh(half) + half


def silu(x):
    return silu_of_half(0.5 * x)


def layer_norm(values):
    centre = values - jnp.sum(values, axis=-1, keepdims=True) * (1.0 / D)
    spread = jnp.sum(centre * centre, axis=-1, keepdims=True) * (1.0 / D)
    return centre * lax.rsqrt(spread + EPSILON)


def split_high_low(values):
    high = values.astype(BF16).astype(F32)
    return high, (values - high).astype(BF16).astype(F32)


def store_rows(table, first, values):
    rows = values.shape[0]
    for part in range(PARTS):
        table[pl.ds(first * PARTS + part, rows, stride=PARTS), :] = values[
            :, part * LANES : (part + 1) * LANES
        ]


def load_rows(table, first, rows):
    return jnp.concatenate(
        [table[pl.ds(first * PARTS + part, rows, stride=PARTS), :] for part in range(PARTS)],
        axis=1,
    )


def kernel(
    grid_send_hbm, g2m_sender_hbm, near_lists_hbm, far_lists_hbm, mesh_sender_hbm,
    g2m_receiver_hbm, g2m_geom_hbm, mesh_geom_hbm, mesh_receiver_hbm, mesh_edge_geom_hbm,
    mesh_in_hbm, geo_in_hbm, grid_hbm, embed_hbm, pair_hbm, square_hbm,
    out,
    grid_send, g2m_sender, near_lists, far_lists, mesh_sender,
    g2m_receiver, g2m_geom, mesh_geom, mesh_receiver, mesh_edge_geom, mesh_in, geo_in,
    mesh_rows,
    grid, embed, pair, square,
    table, staged, grid_out, grid_arrived, near_out, near_arrived, far_out, far_arrived,
    geo_x, geo_w, x_grid, x_mesh, y_rows, pre, gathered_0, gathered_1, hidden_0, hidden_1,
    product_0, product_1, message_0, message_1, edge_sum, latent,
    load_sem, grid_ssem, grid_rsem, near_ssem, near_rsem, far_ssem, far_rsem,
):
    lat = lax.axis_index("lat")
    lon = lax.axis_index("lon")
    me = lat * N_LON + lon
    lats = [lax.rem(lat + step, N_LAT) for step in range(N_LAT)]
    lons = [lax.rem(lon + step, N_LON) for step in range(N_LON)]
    others = [(a, b) for a in range(N_LAT) for b in range(N_LON) if a or b]
    gathered, hidden = (gathered_0, gathered_1), (hidden_0, hidden_1)
    product, message = (product_0, product_1), (message_0, message_1)

    loads = [
        pltpu.make_async_copy(source, target, load_sem.at[k])
        for k, (source, target) in enumerate((
            (grid_hbm, grid), (embed_hbm, embed),
            (square_hbm.at[0], square.at[0]), (pair_hbm.at[0, 0], pair.at[0, 0]),
            (grid_send_hbm, grid_send),
            (square_hbm.at[pl.ds(1, 7)], square.at[pl.ds(1, 7)]),
            (pair_hbm.at[0, pl.ds(1, 3)], pair.at[0, pl.ds(1, 3)]),
            (pair_hbm.at[pl.ds(1, 2)], pair.at[pl.ds(1, 2)]),
            (g2m_sender_hbm, g2m_sender), (near_lists_hbm, near_lists), (far_lists_hbm, far_lists),
            (mesh_sender_hbm, mesh_sender), (g2m_receiver_hbm, g2m_receiver), (g2m_geom_hbm, g2m_geom),
            (mesh_geom_hbm, mesh_geom), (mesh_receiver_hbm, mesh_receiver),
            (mesh_edge_geom_hbm, mesh_edge_geom), (mesh_in_hbm, mesh_in), (geo_in_hbm, geo_in),
        ))
    ]
    for load in loads:
        load.start()

    barrier = pltpu.get_barrier_semaphore()

    for a, b in others:
        pl.semaphore_signal(
            barrier, inc=1, device_id=(lats[a], lons[b]), device_id_type=MESH_AXES
        )

    def send_to(offset, source, target, ssem, rsem):
        lat_step, lon_step = offset
        there = lat + lat_step
        copy = pltpu.make_async_remote_copy(
            source, target, ssem, rsem,
            device_id=(there, lax.rem(lon + lon_step + N_LON, N_LON)),
            device_id_type=MESH_AXES,
        )
        return copy, jnp.logical_and(there >= 0, there < N_LAT)

    def source_exists(offset):
        here = lat - offset[0]
        return jnp.logical_and(here >= 0, here < N_LAT)

    for load in loads[:4]:
        load.wait()
    rows_at_once = 256

    def embed_rows(block, carry):
        rows = pl.ds(pl.multiple_of(block * rows_at_once, rows_at_once), rows_at_once)
        first = lax.dot_general(
            grid[:, rows], embed[...], (((0,), (0,)), ((), ())), preferred_element_type=F32
        )
        first = silu(first).astype(BF16)
        grid_latent = layer_norm(matmul(first, square[0])).astype(BF16)
        store_rows(table, block * rows_at_once, 0.5 * matmul(grid_latent, pair[0, 0]))
        return carry

    lax.fori_loop(0, GRID_DEV // rows_at_once, embed_rows, 0)

    def copy_row(target, slot, row):
        target[pl.ds(slot * PARTS, PARTS), :] = table[pl.ds(row * PARTS, PARTS), :]

    def pick(row_of, first, count):
        for k in range(count):
            copy_row(staged, first + k, row_of(k))

    def run_if(condition, offset, act):
        if offset[0] == 0:
            act()
        else:
            pl.when(condition)(act)

    loads[4].wait()
    pl.semaphore_wait(barrier, DEVICES - 1)
    grid_sends = []
    for d, offset in enumerate(GRID_OFFSETS):
        pick(lambda slot, d=d: grid_send[0, d, slot], d * GSLOT, GSLOT)
        grid_out[d] = staged[pl.ds(d * GSLOT * PARTS, GSLOT * PARTS), :].astype(BF16)
        copy, exists = send_to(
            offset, grid_out.at[d], grid_arrived.at[d], grid_ssem.at[d], grid_rsem.at[d]
        )
        run_if(exists, offset, copy.start)
        grid_sends.append((copy, exists, offset))

    def first_rows(rows, senders, at_once):
        def some(block, carry):
            for k in range(at_once):
                slot = block * at_once + k
                rows[slot] = senders[slot] * PARTS
            return carry

        lax.fori_loop(0, EDGES // at_once, some, 0)

    def build_x(x_ref, receiver, geometry):
        high, low = split_high_low(geometry[...])
        geo_x[0:4, :] = high
        geo_x[4:8, :] = low
        geo_x[8:12, :] = high
        geo_x[12:16, :] = jnp.zeros((4, EDGES), F32)
        x_ref[NODES:KX, :] = geo_x[...].astype(BF16)

        def some(block, carry):
            columns = pl.ds(pl.multiple_of(block * CHUNK, CHUNK), CHUNK)
            node = lax.broadcasted_iota(jnp.int32, (NODES, CHUNK), 0)
            x_ref[0:NODES, columns] = jnp.where(node == receiver[:, columns], 1.0, 0.0).astype(BF16)
            return carry

        lax.fori_loop(0, EDGES // CHUNK, some, 0)

    def pre_activation(section, x_ref):
        y_rows[0:NODES, :] = (0.5 * matmul(latent[...], pair[section, 1])).astype(BF16)
        high, low = split_high_low(0.5 * geo_in[section])
        geo_w[0:4, :] = high
        geo_w[4:8, :] = high
        geo_w[8:12, :] = low
        geo_w[12:16, :] = jnp.zeros((4, D), F32)
        y_rows[NODES:KX, :] = geo_w[...].astype(BF16)

        def some(block, carry):
            chunk = pl.ds(pl.multiple_of(block * CHUNK, CHUNK), CHUNK)
            pre[chunk, :] = lax.dot_general(
                x_ref[:, chunk], y_rows[...], (((0,), (0,)), ((), ())), preferred_element_type=F32
            )
            return carry

        lax.fori_loop(0, EDGES // CHUNK, some, 0)

    for load in loads[5:]:
        load.wait()
    build_x(x_grid, g2m_receiver, g2m_geom)
    high, low = split_high_low(mesh_geom[...])
    geo_x[0:3, 0:NODES] = high
    geo_x[3:6, 0:NODES] = low
    geo_x[6:9, 0:NODES] = high
    geo_x[9:16, 0:NODES] = jnp.zeros((7, NODES), F32)
    high, low = split_high_low(mesh_in[...])
    geo_w[0:3, :] = high
    geo_w[3:6, :] = high
    geo_w[6:9, :] = low
    geo_w[9:16, :] = jnp.zeros((7, D), F32)
    mesh_first = lax.dot_general(
        geo_x[:, 0:NODES].astype(BF16), geo_w[...].astype(BF16), (((0,), (0,)), ((), ())),
        preferred_element_type=F32,
    )
    latent[...] = layer_norm(matmul(silu(mesh_first).astype(BF16), square[1])).astype(BF16)
    pre_activation(0, x_grid)

    def edges(section, sender_rows, scale, x_ref):
        chunks = EDGES // CHUNK
        edge_sum[...] = jnp.zeros((NODES, D), F32)

        def gather(block, first, count):
            for slot in range(first, first + count):
                gathered[block % 2][slot * PARTS : (slot + 1) * PARTS, :] = table[
                    pl.ds(sender_rows[block * CHUNK + slot] * scale, PARTS), :
                ]

        def hide(block, first):
            half = pre[pl.ds(block * CHUNK + first, SLICE), :] + load_rows(
                gathered[block % 2], first, SLICE
            )
            hidden[block % 2][first : first + SLICE, :] = silu_of_half(half).astype(BF16)

        def multiply(block, first, count):
            product[block % 2][first : first + count, :] = matmul(
                hidden[block % 2][first : first + count, :], square[2 + 2 * section]
            )

        def normalize(block, first):
            message[block % 2][first : first + SLICE, :] = layer_norm(
                product[block % 2][first : first + SLICE, :]
            ).astype(BF16)

        def add_up(block):
            edge_sum[...] += matmul(
                x_ref[0:NODES, block * CHUNK : (block + 1) * CHUNK], message[block % 2][...]
            )

        gather(0, 0, CHUNK)
        for block in range(chunks + 1):
            for first in range(0, CHUNK, SLICE):
                if block + 1 < chunks:
                    gather(block + 1, first, SLICE)
                if block < chunks:
                    hide(block, first)
                if block >= 1:
                    normalize(block - 1, first)
                if block < chunks and (first + SLICE) % HALF == 0:
                    multiply(block, first + SLICE - HALF, HALF)
            if block >= 1:
                add_up(block - 1)

    def node_update(section):
        before = latent[...]
        first = matmul(before, pair[section, 2]) + matmul(
            edge_sum[...].astype(BF16), pair[section, 3]
        )
        second = layer_norm(matmul(silu(first).astype(BF16), square[3 + 2 * section]))
        return (before.astype(F32) + second).astype(BF16)

    for d, offset in enumerate(GRID_OFFSETS):
        copy = grid_sends[d][0]
        run_if(source_exists(offset), offset, copy.wait_recv)
        table[pl.ds((GRID_DEV + d * GSLOT) * PARTS, GSLOT * PARTS), :] = grid_arrived[d].astype(F32)
    edges(0, g2m_sender, PARTS, x_grid)
    latent[...] = node_update(0)

    def near_copy(step, d):
        return send_to(
            MESH_OFFSETS[d], near_out.at[step, d], near_arrived.at[step, d],
            near_ssem.at[step, d], near_rsem.at[step, d],
        )

    def far_wait(step):
        return pltpu.make_async_remote_copy(
            far_out.at[step, pl.ds(0, DEVICES - 1)], far_arrived.at[step, pl.ds(0, DEVICES - 1)],
            far_ssem.at[step], far_rsem.at[step],
            device_id=(lat, lons[1]), device_id_type=MESH_AXES,
        )

    def processor_step(step, carry):
        section = step + 1
        store_rows(table, 0, 0.5 * matmul(latent[...], pair[section, 0]))
        pick(lambda slot: far_lists[0, slot % FAR, slot // FAR], 0, DEVICES * FAR)
        far_out[step] = staged[0 : DEVICES * FAR * PARTS, :].astype(BF16).reshape(
            DEVICES, FAR * PARTS, LANES
        )
        far_arrived[step, me] = far_out[step, me]
        for n, d in enumerate((0, 1, 2, 5, 6, 7, 3, 4)):
            pick(lambda slot, d=d: near_lists[0, d, slot], n * NEAR, NEAR)
            near_out[step, d] = staged[n * NEAR * PARTS : (n + 1) * NEAR * PARTS, :].astype(BF16)
            if n == 0:
                for a, b in others:
                    pltpu.make_async_remote_copy(
                        far_out.at[step, lats[a] * N_LON + lons[b]], far_arrived.at[step, me],
                        far_ssem.at[step], far_rsem.at[step],
                        device_id=(lats[a], lons[b]), device_id_type=MESH_AXES,
                    ).start()
            copy, exists = near_copy(step, d)
            run_if(exists, MESH_OFFSETS[d], copy.start)

        @pl.when(step == 0)
        def _():
            build_x(x_mesh, mesh_receiver, mesh_edge_geom)
            first_rows(mesh_rows, mesh_sender, 256)

        pre_activation(section, x_mesh)
        for d, offset in enumerate(MESH_OFFSETS):
            run_if(source_exists(offset), offset, near_copy(step, d)[0].wait_recv)
            table[pl.ds((NODES + d * NEAR) * PARTS, NEAR * PARTS), :] = near_arrived[step, d].astype(
                F32
            )
        far_wait(step).wait_recv()
        table[pl.ds((NODES + NEAR_ROWS) * PARTS, DEVICES * FAR * PARTS), :] = far_arrived[
            step
        ].astype(F32).reshape(DEVICES * FAR * PARTS, LANES)
        edges(section, mesh_rows, 1, x_mesh)
        latent[...] = node_update(section)
        return carry

    lax.fori_loop(0, 2, processor_step, 0)
    out[...] = latent[...]
    for copy, exists, offset in grid_sends:
        run_if(exists, offset, copy.wait_send)
    for step in range(2):
        for d, offset in enumerate(MESH_OFFSETS):
            copy, exists = near_copy(step, d)
            run_if(exists, offset, copy.wait_send)
        far_wait(step).wait_send()


def per_device(
    grid_feat, grid_send, g2m_sender, g2m_receiver, g2m_geom, mesh_geom, mesh_adjacent_lists,
    mesh_far, mesh_sender, mesh_receiver, mesh_edge_geom, embed_in, mesh_in, geo_in, pair_in,
    square_out,
):
    vmem = pl.BlockSpec(memory_space=pltpu.VMEM)
    hbm = pl.BlockSpec(memory_space=pl.ANY)
    dma = pltpu.SemaphoreType.DMA
    return pl.pallas_call(
        kernel,
        out_shape=jax.ShapeDtypeStruct((NODES, D), BF16),
        in_specs=[hbm] * 16,
        out_specs=vmem,
        scratch_shapes=[
            pltpu.SMEM((1, 4, GSLOT), jnp.int32), pltpu.SMEM((EDGES,), jnp.int32),
            pltpu.SMEM((1, 8, NEAR), jnp.int32), pltpu.SMEM((1, FAR, DEVICES), jnp.int32),
            pltpu.SMEM((EDGES,), jnp.int32),
            pltpu.VMEM((1, EDGES), jnp.int32), pltpu.VMEM((4, EDGES), F32),
            pltpu.VMEM((3, NODES), F32), pltpu.VMEM((1, EDGES), jnp.int32),
            pltpu.VMEM((4, EDGES), F32), pltpu.VMEM((3, D), F32), pltpu.VMEM((3, 4, D), F32),
            pltpu.SMEM((EDGES,), jnp.int32),
            pltpu.VMEM((C_IN, GRID_DEV), BF16),
            pltpu.VMEM((C_IN, D), BF16),
            pltpu.VMEM((3, 4, D, D), BF16),
            pltpu.VMEM((8, D, D), BF16),
            pltpu.VMEM(((GRID_DEV + 4 * GSLOT) * PARTS, LANES), F32),
            pltpu.VMEM((4 * GSLOT * PARTS, LANES), F32),
            pltpu.VMEM((4, GSLOT * PARTS, LANES), BF16),
            pltpu.VMEM((4, GSLOT * PARTS, LANES), BF16),
            pltpu.VMEM((2, 8, NEAR * PARTS, LANES), BF16),
            pltpu.VMEM((2, 8, NEAR * PARTS, LANES), BF16),
            pltpu.VMEM((2, DEVICES, FAR * PARTS, LANES), BF16),
            pltpu.VMEM((2, DEVICES, FAR * PARTS, LANES), BF16),
            pltpu.VMEM((16, EDGES), F32),
            pltpu.VMEM((16, D), F32),
            pltpu.VMEM((KX, EDGES), BF16),
            pltpu.VMEM((KX, EDGES), BF16),
            pltpu.VMEM((KX, D), BF16),
            pltpu.VMEM((EDGES, D), F32),
            pltpu.VMEM((CHUNK * PARTS, LANES), F32), pltpu.VMEM((CHUNK * PARTS, LANES), F32),
            pltpu.VMEM((CHUNK, D), BF16), pltpu.VMEM((CHUNK, D), BF16),
            pltpu.VMEM((CHUNK, D), F32), pltpu.VMEM((CHUNK, D), F32),
            pltpu.VMEM((CHUNK, D), BF16), pltpu.VMEM((CHUNK, D), BF16),
            pltpu.VMEM((NODES, D), F32),
            pltpu.VMEM((NODES, D), BF16),
            dma((19,)), dma((4,)), dma((4,)), dma((2, 8)), dma((2, 8)), dma((2,)), dma((2,)),
        ],
        compiler_params=pltpu.CompilerParams(
            collective_id=0, has_side_effects=True, vmem_limit_bytes=62 * 1024 * 1024
        ),
        name="encoder_processor",
    )(
        grid_send, g2m_sender, mesh_adjacent_lists, jnp.swapaxes(mesh_far, 1, 2), mesh_sender,
        g2m_receiver.reshape(1, EDGES), g2m_geom, mesh_geom, mesh_receiver.reshape(1, EDGES),
        mesh_edge_geom, mesh_in, geo_in,
        grid_feat.T, embed_in, pair_in, square_out,
    )


def solution(mesh):
    split = ("lat", "lon")
    in_specs = (
        P(split, None), P(split, None, None), P(split), P(split), P(None, split), P(None, split),
        P(split, None, None), P(split, None, None), P(split), P(split), P(None, split),
        P(), P(), P(), P(), P(),
    )
    return jax.shard_map(
        per_device, mesh=mesh, in_specs=in_specs, out_specs=P(split, None), check_vma=False
    )
```

```python
import jax
import jax.numpy as jnp
from jax import lax
from jax.experimental import pallas as pl
from jax.experimental.pallas import tpu as pltpu
from jax.sharding import PartitionSpec as P

EPSILON = 1e-05
GRID_OFFSETS = ((-1, 0), (1, 0), (0, -1), (0, 1))
MESH_OFFSETS = ((-1, -1), (-1, 0), (-1, 1), (0, -1), (0, 1), (1, -1), (1, 0), (1, 1))
N_LAT, N_LON = 16, 8
DEVICES = N_LAT * N_LON
D = 512
LANES = 128
PARTS = D // LANES
C_IN = 474
GRID_DEV = 1024
GSLOT = 256
NODES = 320
NEAR = 112
FAR = 4
EDGES = 4096
CHUNK = 512
HALF = CHUNK // 2
SLICE = 32
KX = NODES + 16
NEAR_ROWS = 8 * NEAR
MESH_AXES = pl.DeviceIdType.MESH
BF16, F32 = jnp.bfloat16, jnp.float32


def matmul(left, right):
    return jnp.dot(left, right, preferred_element_type=F32)


def silu_of_half(half):
    return half * jnp.tanh(half) + half


def silu(x):
    return silu_of_half(0.5 * x)


def layer_norm(values):
    centre = values - jnp.sum(values, axis=-1, keepdims=True) * (1.0 / D)
    spread = jnp.sum(centre * centre, axis=-1, keepdims=True) * (1.0 / D)
    return centre * lax.rsqrt(spread + EPSILON)


def scale_to_unit(centred):
    spread = jnp.sum(centred * centred, axis=-1, keepdims=True) * (1.0 / D)
    return centred * lax.rsqrt(spread + EPSILON)


def split_high_low(values):
    high = values.astype(BF16).astype(F32)
    return high, (values - high).astype(BF16).astype(F32)


def store_rows(table, first, values):
    rows = values.shape[0]
    for part in range(PARTS):
        table[pl.ds(first * PARTS + part, rows, stride=PARTS), :] = values[
            :, part * LANES : (part + 1) * LANES
        ]


def load_rows(table, first, rows):
    return jnp.concatenate(
        [table[pl.ds(first * PARTS + part, rows, stride=PARTS), :] for part in range(PARTS)],
        axis=1,
    )


def kernel(
    grid_send_hbm, g2m_sender_hbm, near_lists_hbm, far_lists_hbm, mesh_sender_hbm,
    g2m_receiver_hbm, g2m_geom_hbm, mesh_geom_hbm, mesh_receiver_hbm, mesh_edge_geom_hbm,
    mesh_in_hbm, geo_in_hbm, grid_hbm, embed_hbm, pair_hbm, square_hbm,
    out,
    grid_send, g2m_sender, near_lists, far_lists, mesh_sender,
    g2m_receiver, g2m_geom, mesh_geom, mesh_receiver, mesh_edge_geom, mesh_in, geo_in,
    mesh_rows,
    grid, embed, pair, square,
    table, staged, grid_out, grid_arrived, near_out, near_arrived, far_out, far_arrived,
    geo_x, geo_w, x_grid, x_mesh, y_rows, pre, gathered_0, gathered_1, hidden_0, hidden_1,
    product_0, product_1, message_0, message_1, edge_sum, latent,
    load_sem, grid_ssem, grid_rsem, near_ssem, near_rsem, far_ssem, far_rsem,
):
    lat = lax.axis_index("lat")
    lon = lax.axis_index("lon")
    me = lat * N_LON + lon
    lats = [lax.rem(lat + step, N_LAT) for step in range(N_LAT)]
    lons = [lax.rem(lon + step, N_LON) for step in range(N_LON)]
    others = [(a, b) for a in range(N_LAT) for b in range(N_LON) if a or b]
    gathered, hidden = (gathered_0, gathered_1), (hidden_0, hidden_1)
    product, message = (product_0, product_1), (message_0, message_1)

    loads = [
        pltpu.make_async_copy(source, target, load_sem.at[k])
        for k, (source, target) in enumerate((
            (grid_hbm, grid), (embed_hbm, embed),
            (square_hbm.at[0], square.at[0]), (pair_hbm.at[0, 0], pair.at[0, 0]),
            (grid_send_hbm, grid_send),
            (square_hbm.at[pl.ds(1, 7)], square.at[pl.ds(1, 7)]),
            (pair_hbm.at[0, pl.ds(1, 3)], pair.at[0, pl.ds(1, 3)]),
            (pair_hbm.at[pl.ds(1, 2)], pair.at[pl.ds(1, 2)]),
            (g2m_sender_hbm, g2m_sender), (near_lists_hbm, near_lists), (far_lists_hbm, far_lists),
            (mesh_sender_hbm, mesh_sender), (g2m_receiver_hbm, g2m_receiver), (g2m_geom_hbm, g2m_geom),
            (mesh_geom_hbm, mesh_geom), (mesh_receiver_hbm, mesh_receiver),
            (mesh_edge_geom_hbm, mesh_edge_geom), (mesh_in_hbm, mesh_in), (geo_in_hbm, geo_in),
        ))
    ]
    for load in loads:
        load.start()

    barrier = pltpu.get_barrier_semaphore()

    for a, b in others:
        pl.semaphore_signal(
            barrier, inc=1, device_id=(lats[a], lons[b]), device_id_type=MESH_AXES
        )

    def send_to(offset, source, target, ssem, rsem):
        lat_step, lon_step = offset
        there = lat + lat_step
        copy = pltpu.make_async_remote_copy(
            source, target, ssem, rsem,
            device_id=(there, lax.rem(lon + lon_step + N_LON, N_LON)),
            device_id_type=MESH_AXES,
        )
        return copy, jnp.logical_and(there >= 0, there < N_LAT)

    def source_exists(offset):
        here = lat - offset[0]
        return jnp.logical_and(here >= 0, here < N_LAT)

    for load in loads[:4]:
        load.wait()
    rows_at_once = 256

    def embed_rows(block, carry):
        rows = pl.ds(pl.multiple_of(block * rows_at_once, rows_at_once), rows_at_once)
        first = lax.dot_general(
            grid[:, rows], embed[...], (((0,), (0,)), ((), ())), preferred_element_type=F32
        )
        first = silu(first).astype(BF16)
        grid_latent = layer_norm(matmul(first, square[0])).astype(BF16)
        store_rows(table, block * rows_at_once, 0.5 * matmul(grid_latent, pair[0, 0]))
        return carry

    lax.fori_loop(0, GRID_DEV // rows_at_once, embed_rows, 0)

    def copy_row(target, slot, row):
        target[pl.ds(slot * PARTS, PARTS), :] = table[pl.ds(row * PARTS, PARTS), :]

    def pick(row_of, first, count):
        for k in range(count):
            copy_row(staged, first + k, row_of(k))

    def run_if(condition, offset, act):
        if offset[0] == 0:
            act()
        else:
            pl.when(condition)(act)

    loads[4].wait()
    pl.semaphore_wait(barrier, DEVICES - 1)
    grid_sends = []
    for d, offset in enumerate(GRID_OFFSETS):
        pick(lambda slot, d=d: grid_send[0, d, slot], d * GSLOT, GSLOT)
        grid_out[d] = staged[pl.ds(d * GSLOT * PARTS, GSLOT * PARTS), :].astype(BF16)
        copy, exists = send_to(
            offset, grid_out.at[d], grid_arrived.at[d], grid_ssem.at[d], grid_rsem.at[d]
        )
        run_if(exists, offset, copy.start)
        grid_sends.append((copy, exists, offset))

    def first_rows(rows, senders, at_once):
        def some(block, carry):
            for k in range(at_once):
                slot = block * at_once + k
                rows[slot] = senders[slot] * PARTS
            return carry

        lax.fori_loop(0, EDGES // at_once, some, 0)

    def build_x(x_ref, receiver, geometry):
        high, low = split_high_low(geometry[...])
        geo_x[0:4, :] = high
        geo_x[4:8, :] = low
        geo_x[8:12, :] = high
        geo_x[12:16, :] = jnp.zeros((4, EDGES), F32)
        x_ref[NODES:KX, :] = geo_x[...].astype(BF16)

        def some(block, carry):
            columns = pl.ds(pl.multiple_of(block * CHUNK, CHUNK), CHUNK)
            node = lax.broadcasted_iota(jnp.int32, (NODES, CHUNK), 0)
            x_ref[0:NODES, columns] = jnp.where(node == receiver[:, columns], 1.0, 0.0).astype(BF16)
            return carry

        lax.fori_loop(0, EDGES // CHUNK, some, 0)

    def pre_activation(section, x_ref):
        y_rows[0:NODES, :] = (0.5 * matmul(latent[...], pair[section, 1])).astype(BF16)
        high, low = split_high_low(0.5 * geo_in[section])
        geo_w[0:4, :] = high
        geo_w[4:8, :] = high
        geo_w[8:12, :] = low
        geo_w[12:16, :] = jnp.zeros((4, D), F32)
        y_rows[NODES:KX, :] = geo_w[...].astype(BF16)

        def some(block, carry):
            chunk = pl.ds(pl.multiple_of(block * CHUNK, CHUNK), CHUNK)
            pre[chunk, :] = lax.dot_general(
                x_ref[:, chunk], y_rows[...], (((0,), (0,)), ((), ())), preferred_element_type=F32
            )
            return carry

        lax.fori_loop(0, EDGES // CHUNK, some, 0)

    for load in loads[5:]:
        load.wait()
    def centre(section, carry):
        weight = square[2 + 2 * section].astype(F32)
        mean = jnp.sum(weight, axis=-1, keepdims=True) * (1.0 / D)
        square[2 + 2 * section] = (weight - mean).astype(BF16)
        return carry

    lax.fori_loop(0, 3, centre, 0)
    build_x(x_grid, g2m_receiver, g2m_geom)
    high, low = split_high_low(mesh_geom[...])
    geo_x[0:3, 0:NODES] = high
    geo_x[3:6, 0:NODES] = low
    geo_x[6:9, 0:NODES] = high
    geo_x[9:16, 0:NODES] = jnp.zeros((7, NODES), F32)
    high, low = split_high_low(mesh_in[...])
    geo_w[0:3, :] = high
    geo_w[3:6, :] = high
    geo_w[6:9, :] = low
    geo_w[9:16, :] = jnp.zeros((7, D), F32)
    mesh_first = lax.dot_general(
        geo_x[:, 0:NODES].astype(BF16), geo_w[...].astype(BF16), (((0,), (0,)), ((), ())),
        preferred_element_type=F32,
    )
    latent[...] = layer_norm(matmul(silu(mesh_first).astype(BF16), square[1])).astype(BF16)
    pre_activation(0, x_grid)

    def edges(section, sender_rows, scale, x_ref):
        chunks = EDGES // CHUNK
        edge_sum[...] = jnp.zeros((NODES, D), F32)

        def gather(block, first, count):
            for slot in range(first, first + count):
                gathered[block % 2][slot * PARTS : (slot + 1) * PARTS, :] = table[
                    pl.ds(sender_rows[block * CHUNK + slot] * scale, PARTS), :
                ]

        def hide(block, first):
            half = pre[pl.ds(block * CHUNK + first, SLICE), :] + load_rows(
                gathered[block % 2], first, SLICE
            )
            hidden[block % 2][first : first + SLICE, :] = silu_of_half(half).astype(BF16)

        def multiply(block, first, count):
            product[block % 2][first : first + count, :] = matmul(
                hidden[block % 2][first : first + count, :], square[2 + 2 * section]
            )

        def normalize(block, first):
            message[block % 2][first : first + SLICE, :] = scale_to_unit(
                product[block % 2][first : first + SLICE, :]
            ).astype(BF16)

        def add_up(block):
            edge_sum[...] += matmul(
                x_ref[0:NODES, block * CHUNK : (block + 1) * CHUNK], message[block % 2][...]
            )

        gather(0, 0, CHUNK)
        for block in range(chunks + 1):
            for first in range(0, CHUNK, SLICE):
                if block + 1 < chunks:
                    gather(block + 1, first, SLICE)
                if block < chunks:
                    hide(block, first)
                if block >= 1:
                    normalize(block - 1, first)
                if block < chunks and (first + SLICE) % HALF == 0:
                    multiply(block, first + SLICE - HALF, HALF)
            if block >= 1:
                add_up(block - 1)

    def node_update(section):
        before = latent[...]
        first = matmul(before, pair[section, 2]) + matmul(
            edge_sum[...].astype(BF16), pair[section, 3]
        )
        second = layer_norm(matmul(silu(first).astype(BF16), square[3 + 2 * section]))
        return (before.astype(F32) + second).astype(BF16)

    for d, offset in enumerate(GRID_OFFSETS):
        copy = grid_sends[d][0]
        run_if(source_exists(offset), offset, copy.wait_recv)
        table[pl.ds((GRID_DEV + d * GSLOT) * PARTS, GSLOT * PARTS), :] = grid_arrived[d].astype(F32)
    edges(0, g2m_sender, PARTS, x_grid)
    latent[...] = node_update(0)

    def near_copy(step, d):
        return send_to(
            MESH_OFFSETS[d], near_out.at[step, d], near_arrived.at[step, d],
            near_ssem.at[step, d], near_rsem.at[step, d],
        )

    def far_wait(step):
        return pltpu.make_async_remote_copy(
            far_out.at[step, pl.ds(0, DEVICES - 1)], far_arrived.at[step, pl.ds(0, DEVICES - 1)],
            far_ssem.at[step], far_rsem.at[step],
            device_id=(lat, lons[1]), device_id_type=MESH_AXES,
        )

    def processor_step(step, carry):
        section = step + 1
        store_rows(table, 0, 0.5 * matmul(latent[...], pair[section, 0]))
        pick(lambda slot: far_lists[0, slot % FAR, slot // FAR], 0, DEVICES * FAR)
        far_out[step] = staged[0 : DEVICES * FAR * PARTS, :].astype(BF16).reshape(
            DEVICES, FAR * PARTS, LANES
        )
        far_arrived[step, me] = far_out[step, me]
        for n, d in enumerate((0, 1, 2, 5, 6, 7, 3, 4)):
            pick(lambda slot, d=d: near_lists[0, d, slot], n * NEAR, NEAR)
            near_out[step, d] = staged[n * NEAR * PARTS : (n + 1) * NEAR * PARTS, :].astype(BF16)
            if n == 0:
                for a, b in others:
                    pltpu.make_async_remote_copy(
                        far_out.at[step, lats[a] * N_LON + lons[b]], far_arrived.at[step, me],
                        far_ssem.at[step], far_rsem.at[step],
                        device_id=(lats[a], lons[b]), device_id_type=MESH_AXES,
                    ).start()
            copy, exists = near_copy(step, d)
            run_if(exists, MESH_OFFSETS[d], copy.start)

        @pl.when(step == 0)
        def _():
            build_x(x_mesh, mesh_receiver, mesh_edge_geom)
            first_rows(mesh_rows, mesh_sender, 256)

        pre_activation(section, x_mesh)
        for d, offset in enumerate(MESH_OFFSETS):
            run_if(source_exists(offset), offset, near_copy(step, d)[0].wait_recv)
            table[pl.ds((NODES + d * NEAR) * PARTS, NEAR * PARTS), :] = near_arrived[step, d].astype(
                F32
            )
        far_wait(step).wait_recv()
        table[pl.ds((NODES + NEAR_ROWS) * PARTS, DEVICES * FAR * PARTS), :] = far_arrived[
            step
        ].astype(F32).reshape(DEVICES * FAR * PARTS, LANES)
        edges(section, mesh_rows, 1, x_mesh)
        latent[...] = node_update(section)
        return carry

    lax.fori_loop(0, 2, processor_step, 0)
    out[...] = latent[...]
    for copy, exists, offset in grid_sends:
        run_if(exists, offset, copy.wait_send)
    for step in range(2):
        for d, offset in enumerate(MESH_OFFSETS):
            copy, exists = near_copy(step, d)
            run_if(exists, offset, copy.wait_send)
        far_wait(step).wait_send()


def per_device(
    grid_feat, grid_send, g2m_sender, g2m_receiver, g2m_geom, mesh_geom, mesh_adjacent_lists,
    mesh_far, mesh_sender, mesh_receiver, mesh_edge_geom, embed_in, mesh_in, geo_in, pair_in,
    square_out,
):
    vmem = pl.BlockSpec(memory_space=pltpu.VMEM)
    hbm = pl.BlockSpec(memory_space=pl.ANY)
    dma = pltpu.SemaphoreType.DMA
    return pl.pallas_call(
        kernel,
        out_shape=jax.ShapeDtypeStruct((NODES, D), BF16),
        in_specs=[hbm] * 16,
        out_specs=vmem,
        scratch_shapes=[
            pltpu.SMEM((1, 4, GSLOT), jnp.int32), pltpu.SMEM((EDGES,), jnp.int32),
            pltpu.SMEM((1, 8, NEAR), jnp.int32), pltpu.SMEM((1, FAR, DEVICES), jnp.int32),
            pltpu.SMEM((EDGES,), jnp.int32),
            pltpu.VMEM((1, EDGES), jnp.int32), pltpu.VMEM((4, EDGES), F32),
            pltpu.VMEM((3, NODES), F32), pltpu.VMEM((1, EDGES), jnp.int32),
            pltpu.VMEM((4, EDGES), F32), pltpu.VMEM((3, D), F32), pltpu.VMEM((3, 4, D), F32),
            pltpu.SMEM((EDGES,), jnp.int32),
            pltpu.VMEM((C_IN, GRID_DEV), BF16),
            pltpu.VMEM((C_IN, D), BF16),
            pltpu.VMEM((3, 4, D, D), BF16),
            pltpu.VMEM((8, D, D), BF16),
            pltpu.VMEM(((GRID_DEV + 4 * GSLOT) * PARTS, LANES), F32),
            pltpu.VMEM((4 * GSLOT * PARTS, LANES), F32),
            pltpu.VMEM((4, GSLOT * PARTS, LANES), BF16),
            pltpu.VMEM((4, GSLOT * PARTS, LANES), BF16),
            pltpu.VMEM((2, 8, NEAR * PARTS, LANES), BF16),
            pltpu.VMEM((2, 8, NEAR * PARTS, LANES), BF16),
            pltpu.VMEM((2, DEVICES, FAR * PARTS, LANES), BF16),
            pltpu.VMEM((2, DEVICES, FAR * PARTS, LANES), BF16),
            pltpu.VMEM((16, EDGES), F32),
            pltpu.VMEM((16, D), F32),
            pltpu.VMEM((KX, EDGES), BF16),
            pltpu.VMEM((KX, EDGES), BF16),
            pltpu.VMEM((KX, D), BF16),
            pltpu.VMEM((EDGES, D), F32),
            pltpu.VMEM((CHUNK * PARTS, LANES), F32), pltpu.VMEM((CHUNK * PARTS, LANES), F32),
            pltpu.VMEM((CHUNK, D), BF16), pltpu.VMEM((CHUNK, D), BF16),
            pltpu.VMEM((CHUNK, D), F32), pltpu.VMEM((CHUNK, D), F32),
            pltpu.VMEM((CHUNK, D), BF16), pltpu.VMEM((CHUNK, D), BF16),
            pltpu.VMEM((NODES, D), F32),
            pltpu.VMEM((NODES, D), BF16),
            dma((19,)), dma((4,)), dma((4,)), dma((2, 8)), dma((2, 8)), dma((2,)), dma((2,)),
        ],
        compiler_params=pltpu.CompilerParams(
            collective_id=0, has_side_effects=True, vmem_limit_bytes=62 * 1024 * 1024
        ),
        name="encoder_processor",
    )(
        grid_send, g2m_sender, mesh_adjacent_lists, jnp.swapaxes(mesh_far, 1, 2), mesh_sender,
        g2m_receiver.reshape(1, EDGES), g2m_geom, mesh_geom, mesh_receiver.reshape(1, EDGES),
        mesh_edge_geom, mesh_in, geo_in,
        grid_feat.T, embed_in, pair_in, square_out,
    )


def solution(mesh):
    split = ("lat", "lon")
    in_specs = (
        P(split, None), P(split, None, None), P(split), P(split), P(None, split), P(None, split),
        P(split, None, None), P(split, None, None), P(split), P(split), P(None, split),
        P(), P(), P(), P(), P(),
    )
    return jax.shard_map(
        per_device, mesh=mesh, in_specs=in_specs, out_specs=P(split, None), check_vma=False
    )
```
